32 devices in a mesh: seq: 8 (over y, x, core), head: 4 (over z).
Axes of the slice: x: 2, y: 2, z: 4, core: 2. Of those that a mesh axis runs over, the one named last changes fastest.
Arguments:
- queries: bfloat16 [8192, 6144], P('seq', 'head'), may hold values from -64 to 64
- text: bfloat16 [512, 6144], P(None, 'seq'), may hold values from -6 to 6
- key_weight: bfloat16 [6144, 6144], P('seq', 'head'), may hold values from -0.078125 to 0.078125
- value_weight: bfloat16 [6144, 6144], P('seq', 'head'), may hold values from -0.078125 to 0.078125
- out_grad: bfloat16 [8192, 6144], P('seq', 'head'), may hold values from -6 to 6
Outputs:
- attn_out: bfloat16 [8192, 6144], P('seq', 'head')
- query_grad: bfloat16 [8192, 6144], P('seq', 'head')
- key_weight_grad: float32 [6144, 6144], P('seq', 'head')
- value_weight_grad: float32 [6144, 6144], P('seq', 'head')
- text_grad: float32 [512, 6144], P('head', 'seq')
The draws below stay inside these ranges and needn't reach their ends.
All inputs are finite; a program needn't handle non-finite values.
Results may differ from the reference program's by a relative error of at most 0.006.
The reference program's roundings to bfloat16 on the way (of `probs_low` and `dscores`) count: a program that leaves them out, or rounds other values in their place, can miss the bound.
Values may be sent and summed in bfloat16 or wider, within the bound.
No kernel may reach another device: no remote copies, remote signals or barrier semaphores. Data moves between devices by JAX's collectives and lax.ppermute only.
A program may use at most 128 MiB of HBM per device.

```python
import jax
import jax.numpy as jnp
from jax import lax

D = 6144
HEADS = 48
HS = 128
TEXT = 512
QROWS = 8192


def draw_queries(key, part):
    first = jax.random.fold_in(jax.random.fold_in(key, 7), 0)
    values = jnp.clip(jax.random.normal(first, (QROWS, HEADS * HS), jnp.float32), -6.0, 6.0)
    return values.astype(jnp.bfloat16)


def steps_of(own_key, dims, pieces, low, high):
    level, own = 1.0, jax.random.fold_in(own_key, 6)
    for dim, shards_of in pieces:
        draws = jnp.exp(jax.random.uniform(jax.random.fold_in(own, dim), (shards_of,), jnp.float32, low / len(pieces), high / len(pieces)))
        level = level * jnp.repeat(draws, dims[dim] // shards_of).reshape([-1 if axis == dim else 1 for axis in range(len(dims))])
    return level


def scatter_about(rng, dims, width, most, cuts=(), kind=jnp.bfloat16):
    factor_of = steps_of(rng, dims, cuts, -0.22, 0.18) if cuts else 1.0
    result = jax.random.normal(rng, dims, jnp.float32) * width * factor_of
    return jnp.minimum(jnp.maximum(result, -most), most).astype(kind)


def setup_inputs(seed: int = 0) -> dict:
    splits = jax.random.split(jax.random.key(seed), 6)
    queries = draw_queries(jax.random.fold_in(splits[5], 71), 0)
    text = scatter_about(splits[1], (TEXT, D), 1.0, 6.0, ((1, 8),))
    key_weight = scatter_about(splits[2], (D, HEADS * HS), D ** -0.5, 0.078125, ((0, 8), (1, 4)))
    value_weight = scatter_about(splits[3], (D, HEADS * HS), D ** -0.5, 0.078125, ((0, 8), (1, 4)))
    out_grad = scatter_about(splits[4], (QROWS, HEADS * HS), 1.0, 6.0, ((0, 8), (1, 4)))
    return dict(queries=queries, text=text, key_weight=key_weight, value_weight=value_weight, out_grad=out_grad)


def per_head(items):
    query_head, grad_head, key_head, value_head = items
    score_scale = 1.0 / (HS ** 0.5)
    scores = jnp.dot(query_head, key_head.T, preferred_element_type=jnp.float32) * score_scale
    probs = jax.nn.softmax(scores, axis=-1)
    probs_low = probs.astype(jnp.bfloat16)
    output = jnp.dot(probs_low, value_head, preferred_element_type=jnp.float32).astype(jnp.bfloat16)
    dprobs = jnp.dot(grad_head, value_head.T, preferred_element_type=jnp.float32)
    delta = jnp.sum(probs * dprobs, axis=-1, keepdims=True)
    dscores = (probs * (dprobs - delta) * score_scale).astype(jnp.bfloat16)
    query_part = jnp.dot(dscores, key_head, preferred_element_type=jnp.float32).astype(jnp.bfloat16)
    key_part = jnp.dot(dscores.T, query_head, preferred_element_type=jnp.float32)
    value_part = jnp.dot(probs_low.T, grad_head, preferred_element_type=jnp.float32)
    return output, query_part, key_part, value_part


def split_heads(matrix, count):
    return matrix.reshape(count, HEADS, HS).transpose(1, 0, 2)


def join_heads(stacked, count):
    return stacked.transpose(1, 0, 2).reshape(count, HEADS * HS)


def reference(queries, text, key_weight, value_weight, out_grad):
    key_rows = jnp.dot(text, key_weight, preferred_element_type=jnp.float32).astype(jnp.bfloat16)
    value_rows = jnp.dot(text, value_weight, preferred_element_type=jnp.float32).astype(jnp.bfloat16)
    results = lax.map(per_head, (split_heads(queries, QROWS), split_heads(out_grad, QROWS),
                                 split_heads(key_rows, TEXT), split_heads(value_rows, TEXT)))
    attn_out = join_heads(results[0], QROWS)
    query_grad = join_heads(results[1], QROWS)
    key_grad = join_heads(results[2], TEXT).astype(jnp.bfloat16)
    value_grad = join_heads(results[3], TEXT).astype(jnp.bfloat16)
    key_weight_grad = jnp.dot(text.T, key_grad, preferred_element_type=jnp.float32)
    value_weight_grad = jnp.dot(text.T, value_grad, preferred_element_type=jnp.float32)
    text_grad = (jnp.dot(key_grad, key_weight.T, preferred_element_type=jnp.float32)
                 + jnp.dot(value_grad, value_weight.T, preferred_element_type=jnp.float32))
    return attn_out, query_grad, key_weight_grad, value_weight_grad, text_grad
```

```python
import functools
import math

import jax
import jax.numpy as jnp
from jax import lax
from jax.experimental import pallas as pl
from jax.experimental.pallas import tpu as pltpu
from jax.sharding import PartitionSpec as P

HS = 128
SCALE = 1.0 / HS**0.5
LOG2E = math.log2(math.e)
F32 = jnp.float32
BF16 = jnp.bfloat16
NT = (((1,), (1,)), ((), ()))
NN = (((1,), (0,)), ((), ()))


def dot(a, b, dims=NN):
    return lax.dot_general(a, b, dims, preferred_element_type=F32)


def swap(x, axis, size, bit):
    return lax.ppermute(x, axis, [(j, j ^ (1 << bit)) for j in range(size)])


def mask_of(position, order):
    mask = position * 0
    for k, bit in enumerate(order):
        mask = mask | (((position >> (len(order) - 1 - k)) & 1) << bit)
    return mask


def position_of(mask, order):
    position = mask * 0
    for k, bit in enumerate(order):
        position = position | (((mask >> bit) & 1) << (len(order) - 1 - k))
    return position


def project(text, key_weight, value_weight, blocks, first_col, heads, step_heads):
    tokens, depth = text.shape
    count = blocks.shape[0]
    size = tokens // count
    half = tokens // 2
    cols = step_heads * HS
    steps = heads // step_heads
    offset = first_col // cols

    def body(blocks_ref, text_ref, kw_ref, vw_ref, keep_ref, send_ref, order_ref):
        @pl.when(pl.program_id(0) == 0)
        def _():
            for p in range(count):
                start = pl.multiple_of(blocks_ref[p] * size, size)
                order_ref[p * size : (p + 1) * size, :] = text_ref[pl.ds(start, size), :]

        rows = order_ref[...]
        for index, w_ref in enumerate((kw_ref, vw_ref)):
            part = dot(rows, w_ref[...])
            keep_ref[index] = part[:half]
            send_ref[index] = part[half:]

    shape = jax.ShapeDtypeStruct((2, half, heads * HS), F32)
    block = pl.BlockSpec((2, half, cols), lambda j, b: (0, 0, j))
    weight = pl.BlockSpec((depth, cols), lambda j, b: (0, offset + j))
    return pl.pallas_call(
        body,
        out_shape=(shape, shape),
        grid_spec=pltpu.PrefetchScalarGridSpec(
            num_scalar_prefetch=1,
            grid=(steps,),
            in_specs=[pl.BlockSpec((tokens, depth), lambda j, b: (0, 0)), weight, weight],
            out_specs=[block, block],
            scratch_shapes=[pltpu.VMEM((tokens, depth), BF16)],
        ),
        compiler_params=pltpu.CompilerParams(dimension_semantics=("arbitrary",)),
        cost_estimate=pl.CostEstimate(
            flops=4 * tokens * depth * heads * HS, transcendentals=0, bytes_accessed=0
        ),
        name="project",
    )(blocks, text, key_weight, value_weight)


def attend(queries, out_grad, low, high, first_head, previous):
    rows, width = queries.shape
    half, cols = low.shape[1:]
    heads = cols // HS
    chunk = min(rows, 256)

    def body(q_ref, g_ref, low_ref, high_ref, *refs):
        o_ref, dq_ref, keep_ref, send_ref = refs[-4:]
        k = jnp.concatenate([low_ref[0], high_ref[0]], axis=0)
        v = jnp.concatenate([low_ref[1], high_ref[1]], axis=0)
        k_t = k.T
        v_t = v.T
        dk = None
        dv = None
        for c in range(rows // chunk):
            span = slice(c * chunk, (c + 1) * chunk)
            q = q_ref[span, :]
            g = g_ref[span, :]
            s = dot(k, q, NT)
            top = jnp.max(s, axis=0, keepdims=True)
            e = jnp.exp2((s - top) * (SCALE * LOG2E))
            p = e * (1.0 / jnp.sum(e, axis=0, keepdims=True))
            p_low = p.astype(BF16)
            dp = dot(v, g, NT)
            delta = jnp.sum(p * dp, axis=0, keepdims=True)
            ds = (p * (dp - delta) * SCALE).astype(BF16)
            dv_part = dot(p_low, g)
            dk_part = dot(ds, q)
            dv = dv_part if dv is None else dv + dv_part
            dk = dk_part if dk is None else dk + dk_part
            o_ref[span, :] = dot(v_t, p_low).astype(BF16).T
            dq_ref[span, :] = dot(k_t, ds).astype(BF16).T
        keep_ref[0] = dk[:half]
        keep_ref[1] = dv[:half]
        send_ref[0] = dk[half:].astype(BF16)
        send_ref[1] = dv[half:].astype(BF16)

    wide = pl.BlockSpec((rows, HS), lambda h: (0, first_head + h))
    narrow = pl.BlockSpec((2, half, HS), lambda h: (0, 0, h))
    big = jax.ShapeDtypeStruct((rows, width), BF16)
    args = [queries, out_grad, low, high]
    in_specs = [wide, wide, narrow, narrow]
    aliases = {}
    if previous is not None:
        aliases = {len(args): 0, len(args) + 1: 1}
        args += list(previous)
        in_specs += [pl.BlockSpec(memory_space=pl.ANY)] * 2
    return pl.pallas_call(
        body,
        out_shape=(
            big,
            big,
            jax.ShapeDtypeStruct((2, half, cols), F32),
            jax.ShapeDtypeStruct((2, half, cols), BF16),
        ),
        grid=(heads,),
        in_specs=in_specs,
        out_specs=[wide, wide, narrow, narrow],
        input_output_aliases=aliases,
        compiler_params=pltpu.CompilerParams(dimension_semantics=("arbitrary",)),
        cost_estimate=pl.CostEstimate(
            flops=24 * rows * half * cols, transcendentals=0, bytes_accessed=0
        ),
        name="attend",
    )(*args)


def text_grads(key_weight, value_weight, low, high, places, size, first_col, step_heads, previous):
    depth = key_weight.shape[0]
    half, total = low.shape[1:]
    tokens = 2 * half
    cols = step_heads * HS
    offset = first_col // cols

    def body(places_ref, kw_ref, vw_ref, low_ref, high_ref, *refs):
        out_ref = refs[-1]

        @pl.when(pl.program_id(0) == 0)
        def _():
            out_ref[...] = jnp.zeros_like(out_ref) if previous is None else refs[0][...]

        for side, ref in enumerate((low_ref, high_ref)):
            part = dot(ref[0], kw_ref[...], NT) + dot(ref[1], vw_ref[...], NT)
            for j in range(half // size):
                start = pl.multiple_of(places_ref[side * (half // size) + j] * size, size)
                out_ref[pl.ds(start, size), :] += part[j * size : (j + 1) * size]

    weight = pl.BlockSpec((depth, cols), lambda j, a: (0, offset + j))
    narrow = pl.BlockSpec((2, half, cols), lambda j, a: (0, 0, j))
    fixed = pl.BlockSpec((tokens, depth), lambda j, a: (0, 0))
    return pl.pallas_call(
        body,
        out_shape=jax.ShapeDtypeStruct((tokens, depth), F32),
        grid_spec=pltpu.PrefetchScalarGridSpec(
            num_scalar_prefetch=1,
            grid=(total // cols,),
            in_specs=[weight, weight, narrow, narrow] + ([] if previous is None else [fixed]),
            out_specs=fixed,
        ),
        compiler_params=pltpu.CompilerParams(dimension_semantics=("arbitrary",)),
        cost_estimate=pl.CostEstimate(
            flops=4 * tokens * depth * total, transcendentals=0, bytes_accessed=0
        ),
        name="text_grads",
    )(places, key_weight, value_weight, low, high, *(() if previous is None else (previous,)))


def weight_grads(text, low, high, blocks, width, first_col, step_heads, previous):
    tokens, depth = text.shape
    half, total = low.shape[1:]
    cols = step_heads * HS
    offset = first_col // cols
    count = blocks.shape[0]
    size = tokens // count

    def body(blocks_ref, text_ref, low_ref, high_ref, *refs):
        kwg_ref, vwg_ref, order_ref, low_t, high_t = refs[-5:]

        @pl.when(pl.program_id(0) == 0)
        def _():
            for p in range(count):
                start = pl.multiple_of(blocks_ref[p] * size, size)
                order_ref[p * size : (p + 1) * size, :] = text_ref[pl.ds(start, size), :]
            low_t[...] = order_ref[:half, :].T
            high_t[...] = order_ref[half:, :].T

        for index, out_ref in enumerate((kwg_ref, vwg_ref)):
            out_ref[...] = dot(low_t[...], low_ref[index]) + dot(high_t[...], high_ref[index])

    big = jax.ShapeDtypeStruct((depth, width), F32)
    weight = pl.BlockSpec((depth, cols), lambda j, a: (0, offset + j))
    narrow = pl.BlockSpec((2, half, cols), lambda j, a: (0, 0, j))
    args = [blocks, text, low, high]
    in_specs = [pl.BlockSpec((tokens, depth), lambda j, a: (0, 0)), narrow, narrow]
    aliases = {}
    if previous is not None:
        aliases = {len(args): 0, len(args) + 1: 1}
        args += list(previous)
        in_specs += [pl.BlockSpec(memory_space=pl.ANY)] * 2
    return pl.pallas_call(
        body,
        out_shape=(big, big),
        grid_spec=pltpu.PrefetchScalarGridSpec(
            num_scalar_prefetch=1,
            grid=(total // cols,),
            in_specs=in_specs,
            out_specs=[weight, weight],
            scratch_shapes=[
                pltpu.VMEM((tokens, depth), BF16),
                pltpu.VMEM((depth, half), BF16),
                pltpu.VMEM((depth, half), BF16),
            ],
        ),
        input_output_aliases=aliases,
        compiler_params=pltpu.CompilerParams(dimension_semantics=("arbitrary",)),
        cost_estimate=pl.CostEstimate(
            flops=4 * tokens * depth * total, transcendentals=0, bytes_accessed=0
        ),
        name="weight_grads",
    )(*args)


def gather_low(share, size, order):
    for bit in order[:0:-1]:
        share = jnp.concatenate([share, swap(share, "seq", size, bit)], axis=1)
    return share, swap(share, "seq", size, order[0])


def sum_rows(keep, send, size, order):
    total = keep + swap(send, "seq", size, order[0])
    for bit in order[1:]:
        half = total.shape[1] // 2
        keys = swap(total[0, half:], "seq", size, bit)
        values = swap(total[1, half:].astype(BF16), "seq", size, bit).astype(F32)
        total = total[:, :half] + jnp.stack([keys, values])
    return total.astype(BF16)


def sum_grads(keep, send, size, order):
    total = keep + swap(send, "seq", size, order[0]).astype(F32)
    for bit in order[1:]:
        half = total.shape[1] // 2
        total = total[:, :half] + swap(total[:, half:].astype(BF16), "seq", size, bit).astype(F32)
    return total.astype(BF16)


def local(seq_size, head_size, queries, text, key_weight, value_weight, out_grad):
    tokens = text.shape[0]
    heads = key_weight.shape[1] // HS
    seq_bits = list(range(seq_size.bit_length() - 1))
    head_bits = list(range(head_size.bit_length() - 1))
    orders = (seq_bits, seq_bits[:1] + seq_bits[:0:-1])
    first = ((heads + 1) // 2, heads // 2)
    starts = (0, first[0])
    step_heads = math.gcd(*first)
    seq_at = lax.axis_index("seq")
    head_at = lax.axis_index("head")
    places = jnp.arange(seq_size, dtype=jnp.int32)

    blocks = [seq_at ^ mask_of(places, order) for order in orders]
    parts = [
        project(text, key_weight, value_weight, block, start * HS, count, step_heads)
        for block, count, start in zip(blocks, first, starts)
    ]
    shares = [sum_rows(*part, seq_size, order) for part, order in zip(parts, orders)]
    halves = [gather_low(share, seq_size, order) for share, order in zip(shares, orders)]

    wide = None
    grads = []
    for half, start in zip(halves, starts):
        *wide, keep, send = attend(queries, out_grad, *half, start, wide)
        grads.append((keep, send))
    shares = [sum_grads(*grad, seq_size, order) for grad, order in zip(grads, orders)]
    halves = [gather_low(share, seq_size, order) for share, order in zip(shares, orders)]

    size = tokens // max(seq_size, head_size)
    slots = jnp.arange(tokens // size, dtype=jnp.int32)
    per_head = tokens // head_size // size
    per_seq = tokens // seq_size // size
    total = None
    for half, block, start in zip(halves, blocks, starts):
        natural = block[slots // per_seq] * per_seq + slots % per_seq
        spot = position_of(head_at ^ (natural // per_head), head_bits)
        target = spot * per_head + natural % per_head
        total = text_grads(
            key_weight, value_weight, *half, target, size, start * HS, step_heads, total
        )
    weights = None
    for half, block, start in zip(halves, blocks, starts):
        weights = weight_grads(text, *half, block, heads * HS, start * HS, step_heads, weights)
    for bit in head_bits:
        half = total.shape[0] // 2
        total = total[:half] + swap(total[half:].astype(BF16), "head", head_size, bit).astype(F32)
    return (*wide, *weights, total)


def solution(mesh):
    in_specs = (
        P("seq", "head"),
        P(None, "seq"),
        P("seq", "head"),
        P("seq", "head"),
        P("seq", "head"),
    )
    out_specs = (
        P("seq", "head"),
        P("seq", "head"),
        P("seq", "head"),
        P("seq", "head"),
        P("head", "seq"),
    )
    body = functools.partial(local, mesh.shape["seq"], mesh.shape["head"])
    return jax.shard_map(body, mesh=mesh, in_specs=in_specs, out_specs=out_specs, check_vma=False)
```
